32 devices in a mesh: data: 1 (over z), seq: 32 (over y, x, core).
Axes of the slice: x: 4, y: 4, z: 1, core: 2. Of those that a mesh axis runs over, the one named last changes fastest.
The devices are a block of a 4x4x8 slice.
Arguments:
- act_in: bfloat16 [32, 1024, 1024], P('data', 'seq')
- ln1_scale: float32 [1024], replicated
- ln1_bias: float32 [1024], replicated
- w_in: bfloat16 [1024, 4096], replicated
- b_in: float32 [4096], replicated
- ln2_scale: float32 [2048], replicated
- ln2_bias: float32 [2048], replicated
- w_spatial: bfloat16 [1024, 1024], replicated
- b_spatial: float32 [1024], replicated
- causal_mask: int32 [1024, 1024], replicated
- w_out: bfloat16 [2048, 1024], replicated
- b_out: float32 [1024], replicated
Outputs:
- output: bfloat16 [32, 1024, 1024], P('data', 'seq')
All inputs are finite; a program needn't handle non-finite values.
Results may differ from the reference program's by a relative error of at most 0.0115154.
Values are sent between devices in bfloat16 or wider.
A program may use at most 768 MiB of HBM per device.

```python
import jax
import jax.numpy as jnp
from jax import lax

BATCH_ROWS = 32
SEQ_LEN = 1024
MODEL_DIM = 1024
FFN_DIM = 4096
GATE_DIM = FFN_DIM // 2
LN_EPS = 1e-6


def layer_norm(features, ln_gain, ln_shift):
    mean_val = jnp.mean(features, axis=-1, keepdims=True)
    centered = features - mean_val
    var_val = jnp.mean(centered * centered, axis=-1, keepdims=True)
    return centered * lax.rsqrt(var_val + LN_EPS) * ln_gain + ln_shift


def draw_mask(mask_key):
    cut_points = jax.random.randint(mask_key, (2,), 1, SEQ_LEN)
    positions = jnp.arange(SEQ_LEN)
    doc_id = jnp.sum(positions[:, None] >= cut_points[None, :], axis=1)
    keep_mask = (positions[None, :] <= positions[:, None]) & (doc_id[None, :] == doc_id[:, None])
    return keep_mask.astype(jnp.int32)


def setup_inputs(seed: int = 0, part: int = 0) -> dict:
    key_list = jax.random.split(jax.random.key(seed), 12)
    x_key = jax.random.fold_in(key_list[0], part)
    causal_mask = draw_mask(key_list[7])
    row_count = jnp.sum(causal_mask, axis=1).astype(jnp.float32)
    act_in = jax.random.normal(x_key, (BATCH_ROWS, SEQ_LEN, MODEL_DIM), jnp.float32)
    ln1_scale = 1.0 + 0.5 * jax.random.normal(key_list[1], (MODEL_DIM,), jnp.float32)
    ln1_bias = 0.5 * jax.random.normal(key_list[2], (MODEL_DIM,), jnp.float32)
    w_in = jax.random.normal(key_list[3], (MODEL_DIM, FFN_DIM), jnp.float32) * MODEL_DIM ** -0.5
    b_in = 0.5 * jax.random.normal(key_list[4], (FFN_DIM,), jnp.float32)
    ln2_scale = 1.0 + 0.5 * jax.random.normal(key_list[5], (GATE_DIM,), jnp.float32)
    ln2_bias = 0.5 * jax.random.normal(key_list[6], (GATE_DIM,), jnp.float32)
    w_spatial = jax.random.normal(key_list[8], (SEQ_LEN, SEQ_LEN), jnp.float32) * lax.rsqrt(row_count)[:, None]
    b_spatial = 1.0 + 0.8 * jax.random.normal(key_list[9], (SEQ_LEN,), jnp.float32)
    w_out = jax.random.normal(key_list[10], (GATE_DIM, MODEL_DIM), jnp.float32) * (2.0 * GATE_DIM ** -0.5)
    b_out = 0.3 * jax.random.normal(key_list[11], (MODEL_DIM,), jnp.float32)
    return dict(
        act_in=act_in.astype(jnp.bfloat16),
        ln1_scale=ln1_scale,
        ln1_bias=ln1_bias,
        w_in=w_in.astype(jnp.bfloat16),
        b_in=b_in,
        ln2_scale=ln2_scale,
        ln2_bias=ln2_bias,
        w_spatial=w_spatial.astype(jnp.bfloat16),
        b_spatial=b_spatial,
        causal_mask=causal_mask,
        w_out=w_out.astype(jnp.bfloat16),
        b_out=b_out,
    )


def reference(act_in, ln1_scale, ln1_bias, w_in, b_in, ln2_scale, ln2_bias, w_spatial, b_spatial, causal_mask, w_out, b_out):
    w_masked = jnp.where(causal_mask > 0, w_spatial, jnp.zeros_like(w_spatial))

    def one_sequence(seq_act):
        normed = layer_norm(seq_act.astype(jnp.float32), ln1_scale, ln1_bias).astype(jnp.bfloat16)
        hidden = jax.nn.gelu(jnp.dot(normed, w_in, preferred_element_type=jnp.float32) + b_in, approximate=True).astype(jnp.bfloat16)
        gate_half = hidden[:, :GATE_DIM]
        value_norm = layer_norm(hidden[:, GATE_DIM:].astype(jnp.float32), ln2_scale, ln2_bias).astype(jnp.bfloat16)
        spatial = (jnp.dot(w_masked, value_norm, preferred_element_type=jnp.float32) + b_spatial[:, None]).astype(jnp.bfloat16)
        gated_act = (gate_half.astype(jnp.float32) * spatial.astype(jnp.float32)).astype(jnp.bfloat16)
        projected = jnp.dot(gated_act, w_out, preferred_element_type=jnp.float32) + b_out
        return (seq_act.astype(jnp.float32) + projected).astype(jnp.bfloat16)

    return lax.map(one_sequence, act_in)
```

```python
import jax
import jax.numpy as jnp
from jax import lax
from jax.sharding import PartitionSpec as P

LN_EPS = 1e-6


def layer_norm(features, ln_gain, ln_shift):
    mean_val = jnp.mean(features, axis=-1, keepdims=True)
    centered = features - mean_val
    var_val = jnp.mean(centered * centered, axis=-1, keepdims=True)
    return centered * lax.rsqrt(var_val + LN_EPS) * ln_gain + ln_shift


def solution(mesh):
    row_spec = P('data', 'seq', None)
    replicated = P()

    def local_block(act_in, ln1_scale, ln1_bias, w_in, b_in, ln2_scale, ln2_bias, w_spatial, b_spatial, causal_mask, w_out, b_out):
        gate_dim = w_out.shape[0]
        normed = layer_norm(act_in.astype(jnp.float32), ln1_scale, ln1_bias).astype(jnp.bfloat16)
        hidden = jax.nn.gelu(jnp.einsum('bsd,df->bsf', normed, w_in, preferred_element_type=jnp.float32) + b_in, approximate=True).astype(jnp.bfloat16)
        gate_half = hidden[:, :, :gate_dim]
        value_norm = layer_norm(hidden[:, :, gate_dim:].astype(jnp.float32), ln2_scale, ln2_bias).astype(jnp.bfloat16)
        value_seq = lax.all_to_all(value_norm, 'seq', 0, 1, tiled=True)
        w_masked = jnp.where(causal_mask > 0, w_spatial, jnp.zeros_like(w_spatial))
        spatial_seq = (jnp.einsum('ij,bjc->bic', w_masked, value_seq, preferred_element_type=jnp.float32) + b_spatial[None, :, None]).astype(jnp.bfloat16)
        spatial_rows = lax.all_to_all(spatial_seq, 'seq', 1, 0, tiled=True)
        gated_act = (gate_half.astype(jnp.float32) * spatial_rows.astype(jnp.float32)).astype(jnp.bfloat16)
        projected = jnp.einsum('bsc,cd->bsd', gated_act, w_out, preferred_element_type=jnp.float32) + b_out
        return (act_in.astype(jnp.float32) + projected).astype(jnp.bfloat16)

    return jax.shard_map(local_block, mesh=mesh, in_specs=(row_spec,) + (replicated,) * 11, out_specs=row_spec, check_vma=False)
```

```python
import functools
import math

import jax
import jax.numpy as jnp
from jax import lax
from jax.experimental import pallas as pl
from jax.experimental.pallas import tpu as pltpu
from jax.sharding import PartitionSpec as P

LN_EPS = 1e-6
MESH = pl.DeviceIdType.MESH
F32 = jnp.float32
BF16 = jnp.bfloat16
CORES = 2
NB = 256
GELU_A = math.sqrt(2.0 / math.pi)


def gelu(a):
    return (0.5 * a) * (1.0 + jnp.tanh(a * (GELU_A + (GELU_A * 0.044715) * (a * a))))


def dot(a, b):
    return jnp.dot(a, b, preferred_element_type=F32)


def kernel(n, side, x_hbm, ln1g, ln1b, wi_hbm, b_in, ln2g, ln2b, ws_hbm, bsp, mk_hbm, wo_hbm, b_out, out_hbm,
           xb, u, wv, wg, wo, wm, mk, vbuf, vn, vall, sb, sr, g, st, acc, bcol, q, ob,
           xsem, vsem, msem, gsem, osem, outsem, st_send, st_recv, dir_send, fw_send, fin):
    me = lax.axis_index("seq")
    c = me % CORES
    x = (me // CORES) % side
    y = me // (CORES * side)
    pos = xb.shape[0] // n
    crows = pos * CORES * side
    dim = xb.shape[1]
    gate = wo.shape[0]
    half = gate // 2
    nrel = side - 1

    def dev(yy, xx, cc):
        return (yy * side + xx) * CORES + cc

    def yof(j):
        return (y + j + 1) % side

    def rows_of(j):
        return pl.ds(pl.multiple_of(yof(j) * crows, crows), crows)

    def msg(d, k=1):
        return pl.ds(pl.multiple_of(d * pos, pos), k * pos)

    def xcopy(j):
        return pltpu.make_async_copy(x_hbm.at[rows_of(j)], xb.at[rows_of(j)], xsem.at[j])
    nv = 4
    vw = gate // nv

    def vcopy(i):
        return pltpu.make_async_copy(wi_hbm.at[:, pl.ds(gate + i * vw, vw)], wv.at[:, pl.ds(i * vw, vw)], vsem.at[i])
    xcopy(0).start()
    for i in range(nv):
        vcopy(i).start()
    for j in range(1, side):
        xcopy(j).start()
    ws_copy = pltpu.make_async_copy(ws_hbm, wm, msem.at[0])
    mk_copy = pltpu.make_async_copy(mk_hbm, mk, msem.at[1])
    wg_copy = pltpu.make_async_copy(wi_hbm.at[:, pl.ds(0, gate)], wg, gsem)
    wo_copy = pltpu.make_async_copy(wo_hbm, wo, osem)

    barrier = pltpu.get_barrier_semaphore()
    peers = [dev(y, (x + dx) % side, cc) for dx in range(1, side) for cc in range(CORES)]
    peers += [dev((y + dy) % side, x, cc) for dy in range(1, side) for cc in range(CORES)]
    peers += [dev(y, x, 1 - c)]
    for p in peers:
        pl.semaphore_signal(barrier, inc=1, device_id={"seq": p}, device_id_type=MESH)

    def remote(src, dst, ssem, rsem, target):
        return pltpu.make_async_remote_copy(src_ref=src, dst_ref=dst, send_sem=ssem, recv_sem=rsem,
                                            device_id={"seq": target}, device_id_type=MESH)

    srcs, dsts = (vn, sb), (vall, sr)
    other = dev(y, x, 1 - c)

    def send_stage(a, h, j, i, start=True):
        xx = (x + i + 1) % side
        k = nrel * j + i
        cp = remote(srcs[a].at[h, msg(dev(yof(j), xx, 0), CORES)], st.at[a, h, k], st_send.at[a, h, k], st_recv.at[a, h, k],
                    dev(y, xx, c))
        return cp

    def send_direct(a, h, d, k):
        return remote(srcs[a].at[h, msg(d)], dsts[a].at[h, msg(me)], dir_send.at[a, h, k], fin.at[a, h, me], d)

    def directs(j):
        if j < nrel:
            return [(dev(yof(j), x, cc), CORES * j + cc) for cc in range(CORES)]
        base = CORES * nrel
        out = [(dev(y, (x + i + 1) % side, cc), base + CORES * i + cc) for i in range(nrel) for cc in range(CORES)]
        return out + [(other, 2 * base)]

    def send_chunk(a, h, j):
        if j < nrel:
            for i in range(nrel):
                send_stage(a, h, j, i).start()
        for d, k in directs(j):
            send_direct(a, h, d, k).start()

    def forward(a, h, j, i, cc):
        k = nrel * j + i
        origin = dev(y, (x + side - i - 1) % side, c)
        return remote(st.at[a, h, k, pl.ds(cc * pos, pos)], dsts[a].at[h, msg(origin)], fw_send.at[a, h, CORES * k + cc],
                      fin.at[a, h, origin], dev(yof(j), x, cc))

    def relay(a, h, j):
        for i in range(nrel):
            send_stage(a, h, j, i).wait_recv()
            for cc in range(CORES):
                forward(a, h, j, i, cc).start()

    def wait_from(a, h, origin):
        remote(srcs[a].at[h, msg(me)], dsts[a].at[h, msg(origin)], dir_send.at[a, h, 0], fin.at[a, h, origin], other).wait_recv()

    def wait_row(a, h, yy):
        def body(k, carry):
            d = yy * (CORES * side) + k

            @pl.when(d != me)
            def _():
                wait_from(a, h, d)
            return carry
        lax.fori_loop(0, CORES * side, body, 0)

    def own(a, h):
        dsts[a][h, msg(me), :] = srcs[a][h, msg(me), :]

    lnr = 64

    def ln1(j):
        base = yof(j) * crows

        def body(k, carry):
            r = pl.ds(pl.multiple_of(base + k * lnr, lnr), lnr)
            v = xb[r, :].astype(F32)
            cen = v - jnp.sum(v, axis=-1, keepdims=True) * (1.0 / dim)
            var = jnp.sum(cen * cen, axis=-1, keepdims=True) * (1.0 / dim)
            u[r, :] = (cen * lax.rsqrt(var + LN_EPS) * ln1g[...] + ln1b[...]).astype(BF16)
            return carry
        lax.fori_loop(0, crows // lnr, body, 0, unroll=2)

    def value_cols(j, lo, hi):
        rows = rows_of(j)

        def body(b, carry):
            cols = pl.ds(pl.multiple_of(b * NB, NB), NB)
            bcols = pl.ds(pl.multiple_of(gate + b * NB, NB), NB)
            vbuf[:, cols] = gelu(dot(u[rows, :], wv[:, cols]) + b_in[:, bcols]).astype(BF16)
            return carry
        lax.fori_loop(lo, hi, body, 0)

    lnr2 = 32

    def ln2(j):
        base = yof(j) * crows

        def body(k, carry):
            r0 = pl.multiple_of(k * lnr2, lnr2)
            v = vbuf[pl.ds(r0, lnr2), :].astype(F32)
            cen = v - jnp.sum(v, axis=-1, keepdims=True) * (1.0 / gate)
            var = jnp.sum(cen * cen, axis=-1, keepdims=True) * (1.0 / gate)
            o = (cen * lax.rsqrt(var + LN_EPS) * ln2g[...] + ln2b[...]).astype(BF16)
            r = pl.ds(pl.multiple_of(base + r0, lnr2), lnr2)
            vn[0, r, :] = o[:, :half]
            vn[1, r, :] = o[:, half:]
            return carry
        lax.fori_loop(0, crows // lnr2, body, 0, unroll=2)

    def gate_chunk(j):
        rows = rows_of(j)
        for h in range(2):
            def body(b, carry):
                cols = pl.ds(pl.multiple_of(b * NB, NB), NB)
                wcols = pl.ds(pl.multiple_of(h * half + b * NB, NB), NB)
                g[h, rows, cols] = gelu(dot(u[rows, :], wg[:, wcols]) + b_in[:, wcols]).astype(BF16)
                return carry
            lax.fori_loop(0, half // NB, body, 0)

    def mask_weights():
        step = 64

        def body(k, carry):
            r = pl.ds(pl.multiple_of(k * step, step), step)
            wm[r, :] = jnp.where(mk[r, :] > 0, wm[r, :].astype(F32), 0.0).astype(BF16)
            return carry
        lax.fori_loop(0, wm.shape[0] // step, body, 0)
        for k in range(bsp.shape[1] // 128):
            blk = jnp.broadcast_to(bsp[:, k * 128:(k + 1) * 128], (128, 128))
            bcol[k * 128:(k + 1) * 128, :] = blk.T

    def spatial(h, j):
        rows = rows_of(j)

        def body(b, carry):
            cols = pl.ds(pl.multiple_of(b * NB, NB), NB)
            sb[h, rows, cols] = (dot(wm[rows, :], vall[h, :, cols]) + bcol[rows, 0:1]).astype(BF16)
            return carry
        lax.fori_loop(0, half // NB, body, 0)

    def gated(h, rows):
        q[...] = (g[h, rows, :].astype(F32) * sr[h, rows, :].astype(F32)).astype(BF16)

    def arrive(j):
        return (y + side - 1 - j) % side

    def arrive_rows(j):
        return pl.ds(pl.multiple_of(arrive(j) * crows, crows), crows)

    def project0(j):
        rows = arrive_rows(j)
        gated(0, rows)

        def body(b, carry):
            cols = pl.ds(pl.multiple_of(b * NB, NB), NB)
            acc[rows, cols] = dot(q[...], wo[:half, cols]) + (b_out[:, cols] + xb[rows, cols].astype(F32))
            return carry
        lax.fori_loop(0, dim // NB, body, 0)

    def out_copy(j):
        return pltpu.make_async_copy(ob.at[arrive_rows(j)], out_hbm.at[arrive_rows(j)], outsem.at[j])

    def project1(j):
        rows = arrive_rows(j)
        gated(1, rows)

        def body(b, carry):
            cols = pl.ds(pl.multiple_of(b * NB, NB), NB)
            ob[rows, cols] = (acc[rows, cols] + dot(q[...], wo[half:, cols])).astype(BF16)
            return carry
        lax.fori_loop(0, dim // NB, body, 0)
        out_copy(j).start()

    for j in range(side):
        xcopy(j).wait()
        ln1(j)
        if j == 0:
            for i in range(nv):
                vcopy(i).wait()
                value_cols(j, i * vw // NB, (i + 1) * vw // NB)
            ws_copy.start()
            mk_copy.start()
            wg_copy.start()
            wo_copy.start()
        else:
            value_cols(j, 0, gate // NB)
        ln2(j)
        if j == 0:
            pl.semaphore_wait(barrier, len(peers))
        send_chunk(0, 0, j)
        if j >= 2:
            relay(0, 0, j - 2)
    for j in range(side):
        send_chunk(0, 1, j)
    own(0, 0)
    own(0, 1)
    wg_copy.wait()
    gate_chunk(0)
    gate_chunk(1)
    relay(0, 0, 2)
    gate_chunk(2)
    gate_chunk(3)
    ws_copy.wait()
    mk_copy.wait()
    mask_weights()
    wo_copy.wait()
    for j in range(side):
        wait_row(0, 0, arrive(j))
    for j in range(side):
        spatial(0, j)
        send_chunk(1, 0, j)
    own(1, 0)
    for j in range(nrel):
        relay(0, 1, j)
    for j in range(side):
        wait_row(0, 1, arrive(j))
    for j in range(side):
        spatial(1, j)
        send_chunk(1, 1, j)
    own(1, 1)
    for j in range(nrel):
        relay(1, 0, j)
    for j in range(side):
        wait_row(1, 0, arrive(j))
        project0(j)
        if j < nrel:
            relay(1, 1, j)
    for j in range(side):
        wait_row(1, 1, arrive(j))
        project1(j)

    for a in range(2):
        for h in range(2):
            for j in range(nrel):
                for i in range(nrel):
                    send_stage(a, h, j, i).wait_send()
                    for cc in range(CORES):
                        forward(a, h, j, i, cc).wait_send()
            for j in range(side):
                for d, k in directs(j):
                    send_direct(a, h, d, k).wait_send()
    for j in range(side):
        out_copy(j).wait()


def solution(mesh):
    n = mesh.shape['seq']
    side = math.isqrt(n // CORES)
    row_spec = P('data', 'seq', None)
    replicated = P()

    def local_block(act_in, ln1_scale, ln1_bias, w_in, b_in, ln2_scale, ln2_bias, w_spatial, b_spatial, causal_mask, w_out, b_out):
        batch, pos, dim = act_in.shape
        gate = w_out.shape[0]
        half = gate // 2
        rows = batch * pos
        seq_len = w_spatial.shape[0]
        crows = pos * CORES * side
        nrel = side - 1
        if batch != n or side * side * CORES != n:
            raise ValueError('unexpected group')
        vm = pl.BlockSpec(memory_space=pltpu.VMEM)
        anyspec = pl.BlockSpec(memory_space=pl.ANY)
        dma = pltpu.SemaphoreType.DMA
        out = pl.pallas_call(
            functools.partial(kernel, n, side),
            out_shape=jax.ShapeDtypeStruct((rows, dim), BF16),
            in_specs=[anyspec, vm, vm, anyspec, vm, vm, vm, anyspec, vm, anyspec, anyspec, vm],
            out_specs=anyspec,
            scratch_shapes=[
                pltpu.VMEM((rows, dim), BF16), pltpu.VMEM((rows, dim), BF16),
                pltpu.VMEM((dim, gate), BF16), pltpu.VMEM((dim, gate), BF16), pltpu.VMEM((gate, dim), BF16),
                pltpu.VMEM((seq_len, seq_len), BF16), pltpu.VMEM((seq_len, seq_len), jnp.int32),
                pltpu.VMEM((crows, gate), BF16),
                pltpu.VMEM((2, rows, half), BF16), pltpu.VMEM((2, seq_len, half), BF16),
                pltpu.VMEM((2, seq_len, half), BF16), pltpu.VMEM((2, rows, half), BF16),
                pltpu.VMEM((2, rows, half), BF16),
                pltpu.VMEM((2, 2, nrel * nrel, CORES * pos, half), BF16),
                pltpu.VMEM((rows, dim), F32), pltpu.VMEM((seq_len, 128), F32),
                pltpu.VMEM((crows, half), BF16), pltpu.VMEM((rows, dim), BF16),
                dma((side,)), dma((4,)), dma((2,)), dma, dma, dma((side,)),
                dma((2, 2, nrel * nrel)), dma((2, 2, nrel * nrel)), dma((2, 2, 2 * CORES * nrel + 1)),
                dma((2, 2, CORES * nrel * nrel)), dma((2, 2, n)),
            ],
            compiler_params=pltpu.CompilerParams(collective_id=0, has_side_effects=True, vmem_limit_bytes=66900000),
            name='gmlp_block',
        )(act_in.reshape(rows, dim), ln1_scale.reshape(1, -1), ln1_bias.reshape(1, -1), w_in, b_in.reshape(1, -1),
          ln2_scale.reshape(1, -1), ln2_bias.reshape(1, -1), w_spatial, b_spatial.reshape(1, -1), causal_mask, w_out,
          b_out.reshape(1, -1))
        return out.reshape(batch, pos, dim)

    return jax.shard_map(local_block, mesh=mesh, in_specs=(row_spec,) + (replicated,) * 11, out_specs=row_spec, check_vma=False)
```

```python
import functools
import math

import jax
import jax.numpy as jnp
from jax import lax
from jax.experimental import pallas as pl
from jax.experimental.pallas import tpu as pltpu
from jax.sharding import PartitionSpec as P

LN_EPS = 1e-6
MESH = pl.DeviceIdType.MESH
F32 = jnp.float32
BF16 = jnp.bfloat16
CORES = 2
NB = 512
GELU_A = math.sqrt(2.0 / math.pi)


def gelu(a):
    return (0.5 * a) * (1.0 + jnp.tanh(a * (GELU_A + (GELU_A * 0.044715) * (a * a))))


def dot(a, b):
    return jnp.dot(a, b, preferred_element_type=F32)


def slot_offsets(side):
    def rank(o):
        da, db = (min(v, side - v) for v in o)
        two_legs = da > 0 and db > 0
        return (not two_legs, da * db if two_legs else 0, da != 0 or db != 0, da > db, -(da + db), o[0] + o[1] != side, o)
    return sorted(((da, db) for da in range(side) for db in range(side)), key=rank)


def kernel(n, side, x_hbm, ln1g, ln1b, wi_hbm, b_in, ln2g, ln2b, ws_hbm, bsp, mk_hbm, wo_hbm, b_out, out_hbm,
           xa, u, wv, wg, wo, wm, mk, vbuf, vn, g, st, bcol, bslot, q, ob,
           xsem, vsem, wsem, msem, gsem, osem, outsem, st_send, st_recv, dir_send, fw_send, fin):
    me = lax.axis_index("seq")
    c = me % CORES
    x = (me // CORES) % side
    y = me // (CORES * side)
    pos = xa.shape[0] // n
    chip = CORES * pos
    dim = xa.shape[1]
    gate = wo.shape[0]
    slots = slot_offsets(side)
    ns = len(slots)
    nrel = (side - 1) * (side - 1)
    home = slots.index((0, 0))
    fa = x + c * (y - x)
    fb = y + c * (x - y)

    def chip_of(da, db):
        a, b = (fa + da) % side, (fb + db) % side
        yy = b + c * (a - b)
        xx = a + c * (b - a)
        return yy * side + xx

    def dev(da, db, cc):
        return chip_of(da, db) * CORES + cc

    def back(s, same):
        da, db = ((side - v) % side for v in slots[s])
        return slots.index((da, db) if same else (db, da))

    def chip_rows(s):
        return pl.ds(pl.multiple_of(chip_of(*slots[s]) * chip, chip), chip)

    def srows(s, k=1):
        return pl.ds(s * chip, k * chip)

    def sub(s, cc):
        return pl.ds(pl.multiple_of(s * chip + cc * pos, pos), pos)

    def msg(d):
        return pl.ds(pl.multiple_of(d * pos, pos), pos)

    barrier = pltpu.get_barrier_semaphore()
    peers = [dev(d, 0, cc) for d in range(1, side) for cc in range(CORES)]
    peers += [dev(0, d, cc) for d in range(1, side) for cc in range(CORES)]
    peers += [dev(0, 0, 1 - c)]
    for p in peers:
        pl.semaphore_signal(barrier, inc=1, device_id={"seq": p}, device_id_type=MESH)

    def wcopy(s):
        return pltpu.make_async_copy(ws_hbm.at[chip_rows(s)], wm.at[srows(s)], wsem.at[s])

    def mcopy(s):
        return pltpu.make_async_copy(mk_hbm.at[chip_rows(s)], mk.at[srows(s)], msem.at[s])
    own_x = pltpu.make_async_copy(x_hbm.at[msg(me)], xa.at[sub(home, c)], xsem)
    wv_copy = pltpu.make_async_copy(wi_hbm.at[:, pl.ds(gate, gate)], wv, vsem)
    wg_copy = pltpu.make_async_copy(wi_hbm.at[:, pl.ds(0, gate)], wg, gsem)
    wo_copy = pltpu.make_async_copy(wo_hbm, wo, osem)
    own_x.start()
    wv_copy.start()

    def remote(src, dst, ssem, rsem, target):
        return pltpu.make_async_remote_copy(src_ref=src, dst_ref=dst, send_sem=ssem, recv_sem=rsem,
                                            device_id={"seq": target}, device_id_type=MESH)

    def landing(a, origin, r):
        return xa.at[sub(r, origin % CORES)] if a == 0 else out_hbm.at[msg(origin)]

    def stage(a, s):
        da, _ = slots[s]
        src = x_hbm.at[chip_rows(s)] if a == 0 else ob.at[srows(s)]
        return remote(src, st.at[a, s], st_send.at[a, s], st_recv.at[a, s], dev(da, 0, c))

    def to_core(same):
        return c if same else 1 - c

    def direct(a, s, same):
        r = back(s, same)
        cc = to_core(same)
        target = dev(*slots[s], cc)
        src = x_hbm.at[msg(target)] if a == 0 else ob.at[sub(s, cc)]
        return remote(src, landing(a, me, r), dir_send.at[a, CORES * (s - nrel) + same], fin.at[a, CORES * r + c], target)

    def directs(s):
        return (False,) if s == home else (True, False)

    def send(a, ss):
        for s in ss:
            if s < nrel:
                stage(a, s).start()
            else:
                for same in directs(s):
                    direct(a, s, same).start()

    def forward(a, s, same):
        da, db = slots[s]
        cc = to_core(same)
        r = back(s, same)
        origin = dev(side - da, 0, c)
        return remote(st.at[a, s, pl.ds(pl.multiple_of(cc * pos, pos), pos)], landing(a, origin, r),
                      fw_send.at[a, CORES * s + same], fin.at[a, CORES * r + c], dev(0, db, cc))

    relay_at = [0]

    def pump(k):
        for _ in range(k):
            a, s = divmod(relay_at[0], nrel)
            relay_at[0] += 1
            with jax.named_scope(f"r{a}_{s}"):
                stage(a, s).wait_recv()
                for same in (True, False):
                    forward(a, s, same).start()

    def wait_slots(a, ss):
        for r in ss:
            for oc in ([1 - c] if r == home else range(CORES)):
                remote(x_hbm.at[msg(me)], landing(a, dev(*slots[r], oc), r), dir_send.at[a, 0],
                       fin.at[a, CORES * r + oc], dev(0, 0, 1 - c)).wait_recv()

    lnr = 64

    def ln1(ss):
        for s in ss:
            v = xa[srows(s), :].astype(F32)
            cen = v - jnp.sum(v, axis=-1, keepdims=True) * (1.0 / dim)
            var = jnp.sum(cen * cen, axis=-1, keepdims=True) * (1.0 / dim)
            u[srows(s), :] = (cen * lax.rsqrt(var + LN_EPS) * ln1g[...] + ln1b[...]).astype(BF16)

    def value_cols(s0, k):
        def body(b, carry):
            cols = pl.ds(pl.multiple_of(b * NB, NB), NB)
            bcols = pl.ds(pl.multiple_of(gate + b * NB, NB), NB)
            vbuf[0:k * chip, cols] = gelu(dot(u[srows(s0, k), :], wv[:, cols]) + b_in[:, bcols]).astype(BF16)
            return carry
        lax.fori_loop(0, gate // NB, body, 0)

    lnr2 = 32

    def ln2(s0, k):
        for s in range(s0, s0 + k):
            base = chip_of(*slots[s]) * chip

            def body(i, carry):
                v = vbuf[pl.ds(pl.multiple_of((s - s0) * chip + i * lnr2, lnr2), lnr2), :].astype(F32)
                cen = v - jnp.sum(v, axis=-1, keepdims=True) * (1.0 / gate)
                var = jnp.sum(cen * cen, axis=-1, keepdims=True) * (1.0 / gate)
                r = pl.ds(pl.multiple_of(base + i * lnr2, lnr2), lnr2)
                vn[r, :] = (cen * lax.rsqrt(var + LN_EPS) * ln2g[...] + ln2b[...]).astype(BF16)
                return carry
            lax.fori_loop(0, chip // lnr2, body, 0, unroll=True)

    def gate_part(s0, k):
        def body(b, carry):
            cols = pl.ds(pl.multiple_of(b * NB, NB), NB)
            g[srows(s0, k), cols] = gelu(dot(u[srows(s0, k), :], wg[:, cols]) + b_in[:, cols]).astype(BF16)
            return carry
        lax.fori_loop(0, gate // NB, body, 0)

    def mask_weights():
        step = 64

        def body(k, carry):
            r = pl.ds(pl.multiple_of(k * step, step), step)
            wm[r, :] = jnp.where(mk[r, :] > 0, wm[r, :].astype(F32), 0.0).astype(BF16)
            return carry
        lax.fori_loop(0, wm.shape[0] // step, body, 0)
        for k in range(bsp.shape[1] // 128):
            blk = jnp.broadcast_to(bsp[:, k * 128:(k + 1) * 128], (128, 128))
            bcol[k * 128:(k + 1) * 128, :] = blk.T
        for s in range(ns):
            bslot[srows(s), :] = bcol[chip_rows(s), :]

    def spatial(s0, k):
        def body(b, carry):
            cols = pl.ds(pl.multiple_of(b * NB, NB), NB)
            sp = (dot(wm[srows(s0, k), :], vn[:, cols]) + bslot[srows(s0, k), 0:1]).astype(BF16)
            q[0:k * chip, cols] = (g[srows(s0, k), cols].astype(F32) * sp.astype(F32)).astype(BF16)
            return carry
        lax.fori_loop(0, gate // NB, body, 0)

    def project(s0, k):
        rows = srows(s0, k)

        def body(b, carry):
            cols = pl.ds(pl.multiple_of(b * NB, NB), NB)
            ob[rows, cols] = (xa[rows, cols].astype(F32) + (dot(q[0:k * chip, :], wo[:, cols]) + b_out[:, cols])).astype(BF16)
            return carry
        lax.fori_loop(0, dim // NB, body, 0)

    scope = jax.named_scope

    with scope("barrier"):
        pl.semaphore_wait(barrier, len(peers))
    send(0, range(ns))
    wg_copy.start()
    for s in range(ns):
        wcopy(s).start()
        mcopy(s).start()
    wo_copy.start()

    def front(s0, k, pumps=(0, 0, 0), wait_own=False):
        with scope(f"wait0_{s0}"):
            wait_slots(0, range(s0, s0 + k))
        with scope(f"ln1_{s0}"):
            ln1(range(s0, s0 + k))
        pump(pumps[0])
        with scope(f"value_{s0}"):
            value_cols(s0, k)
        pump(pumps[1])
        with scope(f"ln2_{s0}"):
            ln2(s0, k)
        pump(pumps[2])

    with scope("mask"):
        for s in range(ns):
            wcopy(s).wait()
            mcopy(s).wait()
        mask_weights()
    pump(2)
    with scope("w"):
        own_x.wait()
        wv_copy.wait()
        wg_copy.wait()
        wo_copy.wait()
    front(9, 4, (1, 1, 1))
    with scope("gate_9"):
        gate_part(9, 4)
    pump(2)
    front(0, 4, (1, 1, 0))
    with scope("gate_0"):
        gate_part(0, 4)
    front(4, 4)
    front(13, 3)
    front(8, 1)
    done = []
    for i, (s0, k) in enumerate(((0, 2), (2, 2), (4, 4), (8, 4), (12, 4))):
        if s0 == 4:
            with scope("gate_4"):
                gate_part(4, 4)
        if s0 == 8:
            with scope("gate_8"):
                gate_part(8, 1)
        if s0 == 12:
            with scope("gate_13"):
                gate_part(13, 3)
        with scope(f"spatial_{s0}"):
            spatial(s0, k)
        with scope(f"project_{s0}"):
            project(s0, k)
        send(1, range(s0, s0 + k))
        if s0 == 8:
            own_out = pltpu.make_async_copy(ob.at[sub(home, c)], out_hbm.at[msg(me)], outsem)
            own_out.start()
        pump((0, 0, 2, 3, 4)[i])
    assert relay_at[0] == 2 * nrel
    with scope("wait1"):
        wait_slots(1, range(ns))

    with scope("drain"):
        for a in range(2):
            for s in range(ns):
                if s < nrel:
                    stage(a, s).wait_send()
                    for same in (True, False):
                        forward(a, s, same).wait_send()
                else:
                    for same in directs(s):
                        direct(a, s, same).wait_send()
        own_out.wait()


def solution(mesh):
    n = mesh.shape['seq']
    side = math.isqrt(n // CORES)
    row_spec = P('data', 'seq', None)
    replicated = P()

    def local_block(act_in, ln1_scale, ln1_bias, w_in, b_in, ln2_scale, ln2_bias, w_spatial, b_spatial, causal_mask, w_out, b_out):
        batch, pos, dim = act_in.shape
        gate = w_out.shape[0]
        rows = batch * pos
        seq_len = w_spatial.shape[0]
        big = 4 * CORES * pos
        ns = side * side
        nrel = (side - 1) * (side - 1)
        if batch != n or side * side * CORES != n:
            raise ValueError('unexpected group')
        vm = pl.BlockSpec(memory_space=pltpu.VMEM)
        anyspec = pl.BlockSpec(memory_space=pl.ANY)
        dma = pltpu.SemaphoreType.DMA
        out = pl.pallas_call(
            functools.partial(kernel, n, side),
            out_shape=jax.ShapeDtypeStruct((rows, dim), BF16),
            in_specs=[anyspec, vm, vm, anyspec, vm, vm, vm, anyspec, vm, anyspec, anyspec, vm],
            out_specs=anyspec,
            scratch_shapes=[
                pltpu.VMEM((seq_len, dim), BF16), pltpu.VMEM((seq_len, dim), BF16),
                pltpu.VMEM((dim, gate), BF16), pltpu.VMEM((dim, gate), BF16), pltpu.VMEM((gate, dim), BF16),
                pltpu.VMEM((seq_len, seq_len), BF16), pltpu.VMEM((seq_len, seq_len), jnp.int32),
                pltpu.VMEM((big, gate), BF16),
                pltpu.VMEM((seq_len, gate), BF16), pltpu.VMEM((seq_len, gate), BF16),
                pltpu.VMEM((2, nrel, CORES * pos, dim), BF16),
                pltpu.VMEM((seq_len, 128), F32), pltpu.VMEM((seq_len, 128), F32),
                pltpu.VMEM((big, gate), BF16), pltpu.VMEM((seq_len, dim), BF16),
                dma, dma, dma((ns,)), dma((ns,)), dma, dma, dma,
                dma((2, nrel)), dma((2, nrel)), dma((2, CORES * (ns - nrel))),
                dma((2, CORES * nrel)), dma((2, n)),
            ],
            compiler_params=pltpu.CompilerParams(collective_id=0, has_side_effects=True, vmem_limit_bytes=66900000),
            name='gmlp_block',
        )(act_in.reshape(rows, dim), ln1_scale.reshape(1, -1), ln1_bias.reshape(1, -1), w_in, b_in.reshape(1, -1),
          ln2_scale.reshape(1, -1), ln2_bias.reshape(1, -1), w_spatial, b_spatial.reshape(1, -1), causal_mask, w_out,
          b_out.reshape(1, -1))
        return out.reshape(batch, pos, dim)

    return jax.shard_map(local_block, mesh=mesh, in_specs=(row_spec,) + (replicated,) * 11, out_specs=row_spec, check_vma=False)
```

```python
import functools
import math

import jax
import jax.numpy as jnp
from jax import lax
from jax.experimental import pallas as pl
from jax.experimental.pallas import tpu as pltpu
from jax.sharding import PartitionSpec as P

LN_EPS = 1e-6
MESH = pl.DeviceIdType.MESH
F32 = jnp.float32
BF16 = jnp.bfloat16
CORES = 2
NB = 256
GELU_A = math.sqrt(2.0 / math.pi)


def gelu(a):
    return (0.5 * a) * (1.0 + jnp.tanh(a * (GELU_A + (GELU_A * 0.044715) * (a * a))))


def dot(a, b):
    return jnp.dot(a, b, preferred_element_type=F32)


def slot_offsets(side):
    def rank(o):
        da, db = (min(v, side - v) for v in o)
        both = da > 0 and db > 0
        return (not both, da * db if both else 0, da != 0 or db != 0, da > db, da + db, o[0] + o[1] != side, o)
    return sorted(((da, db) for da in range(side) for db in range(side)), key=rank)


def kernel(n, side, x_hbm, ln1g_hbm, ln1b_hbm, wi_hbm, b_in_hbm, ln2g_hbm, ln2b_hbm, ws_hbm, bsp_hbm, mk_hbm, wo_hbm, b_out_hbm,
           out_hbm, ln1g, ln1b, b_in, ln2g, ln2b, bsp, b_out, psem,
           xa, u, wv, wg, wo, wm, mk, vbuf, vn, g, bcol, bslot, q, ob,
           acc0, acc1, xsem, vsem, wsem, msem, gsem, osem, outsem, sent, fin, vx_send, vx_recv):
    me = lax.axis_index("seq")
    c = me % CORES
    x = (me // CORES) % side
    y = me // (CORES * side)
    pos = xa.shape[0] // n
    dim = xa.shape[1]
    gate = wo.shape[0]
    slots = slot_offsets(side)
    ns = len(slots)
    home = slots.index((0, 0))
    seq = ns * pos
    fa = x + c * (y - x)
    fb = y + c * (x - y)

    def chip_of(da, db):
        a, b = (fa + da) % side, (fb + db) % side
        yy = b + c * (a - b)
        xx = a + c * (b - a)
        return yy * side + xx

    def dev(da, db):
        return chip_of(da, db) * CORES + c

    mate = me + 1 - 2 * c

    def back(k):
        return slots.index(tuple((side - v) % side for v in slots[k]))

    def row(s, k):
        return s * seq + k * pos

    def rows(s, k):
        return pl.ds(row(s, k), pos)

    def at(start, size):
        return pl.ds(pl.multiple_of(start, pos), size)

    def seq_rows(chip, s):
        return at((chip * CORES + s) * pos, pos)

    def position(k):
        return at(dev(*slots[k]) * pos, pos)

    barrier = pltpu.get_barrier_semaphore()
    peers = [dev(*o) for o in slots if o != (0, 0)] + [mate]
    for p in peers:
        pl.semaphore_signal(barrier, inc=1, device_id={"seq": p}, device_id_type=MESH)

    wcopies = [pltpu.make_async_copy(ws_hbm.at[position(k)], wm.at[rows(0, k)], wsem.at[k]) for k in range(ns)]
    wcopies += [pltpu.make_async_copy(mk_hbm.at[position(k)], mk.at[rows(0, k)], msem.at[k]) for k in range(ns)]
    own_x = [pltpu.make_async_copy(x_hbm.at[seq_rows(chip_of(0, 0), s)], xa.at[rows(s, home)], xsem.at[s]) for s in range(CORES)]
    own_out = [pltpu.make_async_copy(ob.at[rows(s, home)], out_hbm.at[seq_rows(chip_of(0, 0), s)], outsem.at[s]) for s in range(CORES)]
    wv_copy = pltpu.make_async_copy(wi_hbm.at[:, pl.ds(gate, gate)], wv, vsem)
    wg_copy = pltpu.make_async_copy(wi_hbm.at[:, pl.ds(0, gate)], wg, gsem)
    wo_copy = pltpu.make_async_copy(wo_hbm, wo, osem)
    small = [pltpu.make_async_copy(a, b, psem.at[i]) for i, (a, b) in enumerate((
        (ln1g_hbm, ln1g), (ln1b_hbm, ln1b), (b_in_hbm, b_in), (ln2g_hbm, ln2g), (ln2b_hbm, ln2b), (bsp_hbm, bsp), (b_out_hbm, b_out)))]

    def remote(src, dst, ssem, rsem, target):
        return pltpu.make_async_remote_copy(src_ref=src, dst_ref=dst, send_sem=ssem, recv_sem=rsem,
                                            device_id={"seq": target}, device_id_type=MESH)

    def source(a, s, k):
        return x_hbm.at[seq_rows(chip_of(*slots[k]), s)] if a == 0 else ob.at[rows(s, k)]

    def landing(a, s, k, origin_chip):
        return xa.at[rows(s, k)] if a == 0 else out_hbm.at[seq_rows(origin_chip, s)]

    def message(a, s, k):
        r = back(k)
        return remote(source(a, s, k), landing(a, s, r, chip_of(0, 0)), sent.at[a, s, k], fin.at[a, s, r], dev(*slots[k]))

    def send(a, s, ks):
        for k in ks:
            if k != home:
                message(a, s, k).start()

    def wait_from(a, s, ks):
        for k in ks:
            if k != home:
                remote(source(0, s, home), landing(a, s, k, chip_of(*slots[k])), sent.at[a, s, k], fin.at[a, s, k],
                       mate).wait_recv()

    def swap(s, k):
        return remote(vn.at[s, position(k)], vn.at[s, position(k)], vx_send.at[s, k], vx_recv.at[s, k], mate)

    def wait_swap(s, ks):
        for k in ks:
            da, db = slots[k]
            there = at((chip_of(db, da) * CORES + 1 - c) * pos, pos)
            remote(vn.at[s, position(home)], vn.at[s, there], vx_send.at[s, k], vx_recv.at[s, k], mate).wait_recv()

    accs = (acc0, acc1)
    lnr = 64
    lnr2 = 32

    def ln1(r0, k):
        for r in range(r0, r0 + k, lnr):
            v = xa[r:r + lnr, :].astype(F32)
            cen = v - jnp.sum(v, axis=-1, keepdims=True) * (1.0 / dim)
            var = jnp.sum(cen * cen, axis=-1, keepdims=True) * (1.0 / dim)
            u[r:r + lnr, :] = (cen * lax.rsqrt(var + LN_EPS) * ln1g[...] + ln1b[...]).astype(BF16)

    def steps(hi, product, finish):
        cols = [slice(b, b + NB) for b in range(0, hi, NB)]
        for i in range(len(cols) + 1):
            if i < len(cols):
                raw = product(cols[i])
                k = raw.shape[0]
                accs[i % 2][0:k, :] = raw
            if i > 0:
                finish(cols[i - 1], accs[(i - 1) % 2][0:k, :])

    def value_cols(r0, k):
        def finish(cols, raw):
            bcols = slice(gate + cols.start, gate + cols.stop)
            vbuf[0:k, cols] = gelu(raw + b_in[:, bcols]).astype(BF16)
        steps(gate, lambda cols: dot(u[r0:r0 + k, :], wv[:, cols]), finish)

    def ln2(s, ks):
        for i, k in enumerate(ks):
            v = vbuf[i * pos:(i + 1) * pos, :].astype(F32)
            cen = v - jnp.sum(v, axis=-1, keepdims=True) * (1.0 / gate)
            var = jnp.sum(cen * cen, axis=-1, keepdims=True) * (1.0 / gate)
            vn[s, position(k), :] = (cen * lax.rsqrt(var + LN_EPS) * ln2g[...] + ln2b[...]).astype(BF16)

    def gate_cols(r0, k):
        def finish(cols, raw):
            g[r0:r0 + k, cols] = gelu(raw + b_in[:, cols]).astype(BF16)
        steps(gate, lambda cols: dot(u[r0:r0 + k, :], wg[:, cols]), finish)

    def mask_weights():
        step = 64

        def mask_step(k, carry):
            r = pl.ds(pl.multiple_of(k * step, step), step)
            wm[r, :] = jnp.where(mk[r, :] > 0, wm[r, :].astype(F32), 0.0).astype(BF16)
            return carry
        lax.fori_loop(0, wm.shape[0] // step, mask_step, 0)
        for k in range(bsp.shape[1] // 128):
            blk = jnp.broadcast_to(bsp[:, k * 128:(k + 1) * 128], (128, 128))
            bcol[k * 128:(k + 1) * 128, :] = blk.T
        for k in range(ns):
            bslot[rows(0, k), :] = bcol[position(k), :]

    def spatial(s, w0, k):
        r0 = s * seq + w0

        def finish(cols, raw):
            sp = (raw + bslot[w0:w0 + k, 0:1]).astype(BF16)
            q[0:k, cols] = (g[r0:r0 + k, cols].astype(F32) * sp.astype(F32)).astype(BF16)
        steps(gate, lambda cols: dot(wm[w0:w0 + k, :], vn[s, :, cols]), finish)

    def project(s, w0, k):
        r0 = s * seq + w0

        def finish(cols, raw):
            ob[r0:r0 + k, cols] = (xa[r0:r0 + k, cols].astype(F32) + (raw + b_out[:, cols])).astype(BF16)
        steps(dim, lambda cols: dot(q[0:k, :], wo[:, cols]), finish)

    scope = jax.named_scope

    def front(s, i, k):
        with scope(f"wait0_{s}{i}"):
            if i <= home < i + k:
                own_x[s].wait()
            wait_from(0, s, range(i, i + k))
        with scope(f"ln1_{s}{i}"):
            ln1(s * seq + i * pos, k * pos)
        with scope(f"value_{s}{i}"):
            value_cols(s * seq + i * pos, k * pos)
        with scope(f"ln2_{s}{i}"):
            ln2(s, range(i, i + k))
        for j in range(i, i + k):
            swap(s, j).start()

    def gates(s, i, k):
        with scope(f"gate_{s}{i}"):
            gate_cols(s * seq + i * pos, k * pos)

    def back_part(s, i, k):
        with scope(f"spatial_{s}{i}"):
            spatial(s, i * pos, k * pos)
        with scope(f"project_{s}{i}"):
            project(s, i * pos, k * pos)
        send(1, s, range(i, i + k))
        if i <= home < i + k:
            own_out[s].start()

    for cp in small:
        cp.start()
    for cp in own_x:
        cp.start()
    for cp in wcopies:
        cp.start()
    with scope("barrier"):
        pl.semaphore_wait(barrier, len(peers))
    for s in range(CORES):
        send(0, s, range(ns))
    wv_copy.start()
    wg_copy.start()
    wo_copy.start()
    with scope("mask"):
        for cp in small + wcopies:
            cp.wait()
        mask_weights()
    with scope("w"):
        wv_copy.wait()
        wg_copy.wait()
        wo_copy.wait()
    front(0, 0, 8)
    gates(0, 0, 8)
    front(0, 8, 4)
    front(0, 12, 4)
    gates(0, 8, 8)
    with scope("swap_0"):
        wait_swap(0, range(ns))
    back_part(0, 0, 8)
    back_part(0, 8, 8)
    front(1, 0, 8)
    front(1, 8, 8)
    gates(1, 0, 8)
    gates(1, 8, 8)
    with scope("swap_1"):
        wait_swap(1, range(ns))
    back_part(1, 0, 4)
    back_part(1, 4, 4)
    back_part(1, 8, 4)
    back_part(1, 12, 4)
    with scope("wait1"):
        wait_from(1, 0, range(ns))
        wait_from(1, 1, range(ns))

    with scope("drain"):
        for s in range(CORES):
            for k in range(ns):
                if k != home:
                    for a in range(2):
                        message(a, s, k).wait_send()
                swap(s, k).wait_send()
            own_out[s].wait()


def solution(mesh):
    n = mesh.shape['seq']
    side = math.isqrt(n // CORES)
    row_spec = P('data', 'seq', None)
    replicated = P()

    def local_block(act_in, ln1_scale, ln1_bias, w_in, b_in, ln2_scale, ln2_bias, w_spatial, b_spatial, causal_mask, w_out, b_out):
        batch, pos, dim = act_in.shape
        gate = w_out.shape[0]
        rows = batch * pos
        seq_len = w_spatial.shape[0]
        ns = side * side
        part = 8 * pos
        if batch != n or side * side * CORES != n:
            raise ValueError('unexpected group')
        anyspec = pl.BlockSpec(memory_space=pl.ANY)
        dma = pltpu.SemaphoreType.DMA
        out = pl.pallas_call(
            functools.partial(kernel, n, side),
            out_shape=jax.ShapeDtypeStruct((rows, dim), BF16),
            in_specs=[anyspec] * 12,
            out_specs=anyspec,
            scratch_shapes=[
                pltpu.VMEM((1, dim), F32), pltpu.VMEM((1, dim), F32), pltpu.VMEM((1, 2 * gate), F32), pltpu.VMEM((1, gate), F32),
                pltpu.VMEM((1, gate), F32), pltpu.VMEM((1, seq_len), F32), pltpu.VMEM((1, dim), F32), dma((7,)),
                pltpu.VMEM((rows, dim), BF16), pltpu.VMEM((rows, dim), BF16),
                pltpu.VMEM((dim, gate), BF16), pltpu.VMEM((dim, gate), BF16), pltpu.VMEM((gate, dim), BF16),
                pltpu.VMEM((ns * pos, seq_len), BF16), pltpu.VMEM((ns * pos, seq_len), jnp.int32),
                pltpu.VMEM((part, gate), BF16),
                pltpu.VMEM((CORES, seq_len, gate), BF16), pltpu.VMEM((rows, gate), BF16),
                pltpu.VMEM((seq_len, 128), F32), pltpu.VMEM((ns * pos, 128), F32),
                pltpu.VMEM((part, gate), BF16), pltpu.VMEM((rows, dim), BF16),
                pltpu.VMEM((part, NB), F32), pltpu.VMEM((part, NB), F32),
                dma((CORES,)), dma, dma((ns,)), dma((ns,)), dma, dma, dma((CORES,)),
                dma((2, CORES, ns)), dma((2, CORES, ns)), dma((CORES, ns)), dma((CORES, ns)),
            ],
            compiler_params=pltpu.CompilerParams(collective_id=0, has_side_effects=True, vmem_limit_bytes=66900000),
            name='gmlp_block',
        )(act_in.reshape(rows, dim), ln1_scale.reshape(1, -1), ln1_bias.reshape(1, -1), w_in, b_in.reshape(1, -1),
          ln2_scale.reshape(1, -1), ln2_bias.reshape(1, -1), w_spatial, b_spatial.reshape(1, -1), causal_mask, w_out,
          b_out.reshape(1, -1))
        return out.reshape(batch, pos, dim)

    return jax.shard_map(local_block, mesh=mesh, in_specs=(row_spec,) + (replicated,) * 11, out_specs=row_spec, check_vma=False)
```

```python
import functools
import math

import jax
import jax.numpy as jnp
from jax import lax
from jax.experimental import pallas as pl
from jax.experimental.pallas import tpu as pltpu
from jax.sharding import PartitionSpec as P

LN_EPS = 1e-6
MESH = pl.DeviceIdType.MESH
F32 = jnp.float32
BF16 = jnp.bfloat16
CORES = 2
NB = 256
GELU_A = math.sqrt(2.0 / math.pi)


def gelu(a):
    return (0.5 * a) * (1.0 + jnp.tanh(a * (GELU_A + (GELU_A * 0.044715) * (a * a))))


def dot(a, b):
    return jnp.dot(a, b, preferred_element_type=F32)


def slot_offsets(side):
    def rank(o):
        da, db = (min(v, side - v) for v in o)
        both = da > 0 and db > 0
        return (both, da != 0 or db != 0, da + db, da > db, o[0] + o[1] != side, o)
    return sorted(((da, db) for da in range(side) for db in range(side)), key=rank)


def kernel(n, side, x_hbm, ln1g_hbm, ln1b_hbm, wi_hbm, b_in_hbm, ln2g_hbm, ln2b_hbm, ws_hbm, bsp_hbm, mk_hbm, wo_hbm, b_out_hbm,
           out_hbm, ln1g, ln1b, b_in, ln2g, ln2b, bsp, b_out, psem,
           xa, u, wv, wg, wo, wm, mk, vbuf, vn, g, bcol, bslot, q, ob,
           acc0, acc1, xsem, vsem, wsem, msem, gsem, osem, outsem, sent, fin, vx_send, vx_recv):
    me = lax.axis_index("seq")
    c = me % CORES
    x = (me // CORES) % side
    y = me // (CORES * side)
    pos = xa.shape[0] // n
    dim = xa.shape[1]
    gate = wo.shape[0]
    slots = slot_offsets(side)
    ns = len(slots)
    home = slots.index((0, 0))
    seq = ns * pos
    fa = x + c * (y - x)
    fb = y + c * (x - y)

    def chip_of(da, db):
        a, b = (fa + da) % side, (fb + db) % side
        yy = b + c * (a - b)
        xx = a + c * (b - a)
        return yy * side + xx

    def dev(da, db):
        return chip_of(da, db) * CORES + c

    mate = me + 1 - 2 * c

    def back(k):
        return slots.index(tuple((side - v) % side for v in slots[k]))

    def row(s, k):
        return s * seq + k * pos

    def rows(s, k):
        return pl.ds(row(s, k), pos)

    def at(start, size):
        return pl.ds(pl.multiple_of(start, pos), size)

    def seq_rows(chip, s):
        return at((chip * CORES + s) * pos, pos)

    def position(k):
        return at(dev(*slots[k]) * pos, pos)

    barrier = pltpu.get_barrier_semaphore()
    peers = [dev(*o) for o in slots if o != (0, 0)] + [mate]
    for p in peers:
        pl.semaphore_signal(barrier, inc=1, device_id={"seq": p}, device_id_type=MESH)

    wcopies = [pltpu.make_async_copy(ws_hbm.at[position(k)], wm.at[rows(0, k)], wsem.at[k]) for k in range(ns)]
    wcopies += [pltpu.make_async_copy(mk_hbm.at[position(k)], mk.at[rows(0, k)], msem.at[k]) for k in range(ns)]
    own_x = [pltpu.make_async_copy(x_hbm.at[seq_rows(chip_of(0, 0), s)], xa.at[rows(s, home)], xsem.at[s]) for s in range(CORES)]
    own_out = [pltpu.make_async_copy(ob.at[rows(s, home)], out_hbm.at[seq_rows(chip_of(0, 0), s)], outsem.at[s]) for s in range(CORES)]
    wv_copy = pltpu.make_async_copy(wi_hbm.at[:, pl.ds(gate, gate)], wv, vsem)
    wg_copy = pltpu.make_async_copy(wi_hbm.at[:, pl.ds(0, gate)], wg, gsem)
    wo_copy = pltpu.make_async_copy(wo_hbm, wo, osem)
    small = [pltpu.make_async_copy(a, b, psem.at[i]) for i, (a, b) in enumerate((
        (ln1g_hbm, ln1g), (ln1b_hbm, ln1b), (b_in_hbm, b_in), (ln2g_hbm, ln2g), (ln2b_hbm, ln2b), (bsp_hbm, bsp), (b_out_hbm, b_out)))]

    def remote(src, dst, ssem, rsem, target):
        return pltpu.make_async_remote_copy(src_ref=src, dst_ref=dst, send_sem=ssem, recv_sem=rsem,
                                            device_id={"seq": target}, device_id_type=MESH)

    def source(a, s, k):
        return x_hbm.at[seq_rows(chip_of(*slots[k]), s)] if a == 0 else ob.at[rows(s, k)]

    def landing(a, s, k, origin_chip):
        return xa.at[rows(s, k)] if a == 0 else out_hbm.at[seq_rows(origin_chip, s)]

    def message(a, s, k):
        r = back(k)
        return remote(source(a, s, k), landing(a, s, r, chip_of(0, 0)), sent.at[a, s, k], fin.at[a, s, r], dev(*slots[k]))

    def send(a, s, ks):
        for k in ks:
            if k != home:
                message(a, s, k).start()

    def wait_from(a, s, ks):
        for k in ks:
            if k != home:
                remote(source(0, s, home), landing(a, s, k, chip_of(*slots[k])), sent.at[a, s, k], fin.at[a, s, k],
                       mate).wait_recv()

    def swap(s, k):
        return remote(vn.at[s, position(k)], vn.at[s, position(k)], vx_send.at[s, k], vx_recv.at[s, k], mate)

    def wait_swap(s, ks):
        for k in ks:
            da, db = slots[k]
            there = at((chip_of(db, da) * CORES + 1 - c) * pos, pos)
            remote(vn.at[s, position(home)], vn.at[s, there], vx_send.at[s, k], vx_recv.at[s, k], mate).wait_recv()

    accs = (acc0, acc1)
    lnr = 64
    lnr2 = 32

    def ln1(r0, k):
        for r in range(r0, r0 + k, lnr):
            v = xa[r:r + lnr, :].astype(F32)
            cen = v - jnp.sum(v, axis=-1, keepdims=True) * (1.0 / dim)
            var = jnp.sum(cen * cen, axis=-1, keepdims=True) * (1.0 / dim)
            u[r:r + lnr, :] = (cen * lax.rsqrt(var + LN_EPS) * ln1g[...] + ln1b[...]).astype(BF16)

    def steps(hi, product, finish):
        cols = [slice(b, b + NB) for b in range(0, hi, NB)]
        for i in range(len(cols) + 1):
            if i < len(cols):
                raw = product(cols[i])
                k = raw.shape[0]
                accs[i % 2][0:k, :] = raw
            if i > 0:
                finish(cols[i - 1], accs[(i - 1) % 2][0:k, :])

    def value_cols(r0, k):
        def finish(cols, raw):
            bcols = slice(gate + cols.start, gate + cols.stop)
            vbuf[0:k, cols] = gelu(raw + b_in[:, bcols]).astype(BF16)
        steps(gate, lambda cols: dot(u[r0:r0 + k, :], wv[:, cols]), finish)

    def ln2(s, ks):
        for i, k in enumerate(ks):
            v = vbuf[i * pos:(i + 1) * pos, :].astype(F32)
            cen = v - jnp.sum(v, axis=-1, keepdims=True) * (1.0 / gate)
            var = jnp.sum(cen * cen, axis=-1, keepdims=True) * (1.0 / gate)
            vn[s, position(k), :] = (cen * lax.rsqrt(var + LN_EPS) * ln2g[...] + ln2b[...]).astype(BF16)

    def gate_cols(r0, k):
        def finish(cols, raw):
            g[r0:r0 + k, cols] = gelu(raw + b_in[:, cols]).astype(BF16)
        steps(gate, lambda cols: dot(u[r0:r0 + k, :], wg[:, cols]), finish)

    def mask_weights():
        step = 64

        def mask_step(k, carry):
            r = pl.ds(pl.multiple_of(k * step, step), step)
            wm[r, :] = jnp.where(mk[r, :] > 0, wm[r, :].astype(F32), 0.0).astype(BF16)
            return carry
        lax.fori_loop(0, wm.shape[0] // step, mask_step, 0)
        for k in range(bsp.shape[1] // 128):
            blk = jnp.broadcast_to(bsp[:, k * 128:(k + 1) * 128], (128, 128))
            bcol[k * 128:(k + 1) * 128, :] = blk.T
        for k in range(ns):
            bslot[rows(0, k), :] = bcol[position(k), :]

    def spatial(s, w0, k):
        r0 = s * seq + w0

        def finish(cols, raw):
            sp = (raw + bslot[w0:w0 + k, 0:1]).astype(BF16)
            q[0:k, cols] = (g[r0:r0 + k, cols].astype(F32) * sp.astype(F32)).astype(BF16)
        steps(gate, lambda cols: dot(wm[w0:w0 + k, :], vn[s, :, cols]), finish)

    def project(s, w0, k):
        r0 = s * seq + w0

        def finish(cols, raw):
            ob[r0:r0 + k, cols] = (xa[r0:r0 + k, cols].astype(F32) + (raw + b_out[:, cols])).astype(BF16)
        steps(dim, lambda cols: dot(q[0:k, :], wo[:, cols]), finish)

    scope = jax.named_scope

    def front(s, i, k):
        with scope(f"wait0_{s}{i}"):
            if i <= home < i + k:
                own_x[s].wait()
            wait_from(0, s, range(i, i + k))
        with scope(f"ln1_{s}{i}"):
            ln1(s * seq + i * pos, k * pos)
        with scope(f"value_{s}{i}"):
            value_cols(s * seq + i * pos, k * pos)
        with scope(f"ln2_{s}{i}"):
            ln2(s, range(i, i + k))
        for j in range(i, i + k):
            swap(s, j).start()

    def gates(s, i, k):
        with scope(f"gate_{s}{i}"):
            gate_cols(s * seq + i * pos, k * pos)

    def back_part(s, i, k):
        with scope(f"spatial_{s}{i}"):
            spatial(s, i * pos, k * pos)
        with scope(f"project_{s}{i}"):
            project(s, i * pos, k * pos)
        send(1, s, range(i, i + k))
        if i <= home < i + k:
            own_out[s].start()

    for cp in small:
        cp.start()
    for cp in own_x:
        cp.start()
    for cp in wcopies:
        cp.start()
    wv_copy.start()
    wg_copy.start()
    wo_copy.start()
    with scope("barrier"):
        pl.semaphore_wait(barrier, len(peers))
    for s in range(CORES):
        send(0, s, range(ns))
    with scope("mask"):
        for cp in small + wcopies:
            cp.wait()
        mask_weights()
    with scope("w"):
        wv_copy.wait()
        wg_copy.wait()
        wo_copy.wait()
    front(0, 0, 8)
    gates(0, 0, 8)
    front(0, 8, 4)
    front(0, 12, 4)
    gates(0, 8, 8)
    with scope("swap_0"):
        wait_swap(0, range(ns))
    back_part(0, 8, 4)
    back_part(0, 12, 4)
    back_part(0, 0, 8)
    front(1, 0, 8)
    front(1, 8, 8)
    gates(1, 0, 16)
    with scope("swap_1"):
        wait_swap(1, range(ns))
    back_part(1, 8, 4)
    back_part(1, 12, 4)
    back_part(1, 0, 4)
    back_part(1, 4, 4)
    with scope("wait1"):
        wait_from(1, 0, range(ns))
        wait_from(1, 1, range(ns))

    with scope("drain"):
        for s in range(CORES):
            for k in range(ns):
                if k != home:
                    for a in range(2):
                        message(a, s, k).wait_send()
                swap(s, k).wait_send()
            own_out[s].wait()


def solution(mesh):
    n = mesh.shape['seq']
    side = math.isqrt(n // CORES)
    row_spec = P('data', 'seq', None)
    replicated = P()

    def local_block(act_in, ln1_scale, ln1_bias, w_in, b_in, ln2_scale, ln2_bias, w_spatial, b_spatial, causal_mask, w_out, b_out):
        batch, pos, dim = act_in.shape
        gate = w_out.shape[0]
        rows = batch * pos
        seq_len = w_spatial.shape[0]
        ns = side * side
        part = 16 * pos
        if batch != n or side * side * CORES != n:
            raise ValueError('unexpected group')
        anyspec = pl.BlockSpec(memory_space=pl.ANY)
        dma = pltpu.SemaphoreType.DMA
        out = pl.pallas_call(
            functools.partial(kernel, n, side),
            out_shape=jax.ShapeDtypeStruct((rows, dim), BF16),
            in_specs=[anyspec] * 12,
            out_specs=anyspec,
            scratch_shapes=[
                pltpu.VMEM((1, dim), F32), pltpu.VMEM((1, dim), F32), pltpu.VMEM((1, 2 * gate), F32), pltpu.VMEM((1, gate), F32),
                pltpu.VMEM((1, gate), F32), pltpu.VMEM((1, seq_len), F32), pltpu.VMEM((1, dim), F32), dma((7,)),
                pltpu.VMEM((rows, dim), BF16), pltpu.VMEM((rows, dim), BF16),
                pltpu.VMEM((dim, gate), BF16), pltpu.VMEM((dim, gate), BF16), pltpu.VMEM((gate, dim), BF16),
                pltpu.VMEM((ns * pos, seq_len), BF16), pltpu.VMEM((ns * pos, seq_len), jnp.int32),
                pltpu.VMEM((part, gate), BF16),
                pltpu.VMEM((CORES, seq_len, gate), BF16), pltpu.VMEM((rows, gate), BF16),
                pltpu.VMEM((seq_len, 128), F32), pltpu.VMEM((ns * pos, 128), F32),
                pltpu.VMEM((part, gate), BF16), pltpu.VMEM((rows, dim), BF16),
                pltpu.VMEM((part, NB), F32), pltpu.VMEM((part, NB), F32),
                dma((CORES,)), dma, dma((ns,)), dma((ns,)), dma, dma, dma((CORES,)),
                dma((2, CORES, ns)), dma((2, CORES, ns)), dma((CORES, ns)), dma((CORES, ns)),
            ],
            compiler_params=pltpu.CompilerParams(collective_id=0, has_side_effects=True, vmem_limit_bytes=66900000),
            name='gmlp_block',
        )(act_in.reshape(rows, dim), ln1_scale.reshape(1, -1), ln1_bias.reshape(1, -1), w_in, b_in.reshape(1, -1),
          ln2_scale.reshape(1, -1), ln2_bias.reshape(1, -1), w_spatial, b_spatial.reshape(1, -1), causal_mask, w_out,
          b_out.reshape(1, -1))
        return out.reshape(batch, pos, dim)

    return jax.shard_map(local_block, mesh=mesh, in_specs=(row_spec,) + (replicated,) * 11, out_specs=row_spec, check_vma=False)
```

```python
import functools
import math

import jax
import jax.numpy as jnp
from jax import lax
from jax.experimental import pallas as pl
from jax.experimental.pallas import tpu as pltpu
from jax.sharding import PartitionSpec as P

LN_EPS = 1e-6
MESH = pl.DeviceIdType.MESH
F32 = jnp.float32
BF16 = jnp.bfloat16
CORES = 2
NB = 256
GELU_A = math.sqrt(2.0 / math.pi)


def gelu(a):
    return (0.5 * a) * (1.0 + jnp.tanh(a * (GELU_A + (GELU_A * 0.044715) * (a * a))))


def dot(a, b):
    return jnp.dot(a, b, preferred_element_type=F32)


def slot_offsets(side):
    def rank(o):
        da, db = (min(v, side - v) for v in o)
        both = da > 0 and db > 0
        return (both, da != 0 or db != 0, da + db, da > db, o[0] + o[1] != side, o)
    return sorted(((da, db) for da in range(side) for db in range(side)), key=rank)


def kernel(n, side, x_hbm, ln1g_hbm, ln1b_hbm, wi_hbm, b_in_hbm, ln2g_hbm, ln2b_hbm, ws_hbm, bsp_hbm, mk_hbm, wo_hbm, b_out_hbm,
           out_hbm, ln1g, ln1b, b_in, ln2g, ln2b, bsp, b_out, psem,
           xa, u, wv, wg, wo, wm, mk, vbuf, vn, g, bcol, bslot, q, ob,
           acc0, acc1, xsem, vsem, wsem, msem, gsem, osem, outsem, sent, fin, vx_send, vx_recv):
    me = lax.axis_index("seq")
    c = me % CORES
    x = (me // CORES) % side
    y = me // (CORES * side)
    pos = xa.shape[0] // n
    dim = xa.shape[1]
    gate = wo.shape[0]
    slots = slot_offsets(side)
    ns = len(slots)
    home = slots.index((0, 0))
    seq = ns * pos
    fa = x + c * (y - x)
    fb = y + c * (x - y)

    def chip_of(da, db):
        a, b = (fa + da) % side, (fb + db) % side
        yy = b + c * (a - b)
        xx = a + c * (b - a)
        return yy * side + xx

    def dev(da, db):
        return chip_of(da, db) * CORES + c

    mate = me + 1 - 2 * c

    def back(k):
        return slots.index(tuple((side - v) % side for v in slots[k]))

    def row(s, k):
        return s * seq + k * pos

    def rows(s, k):
        return pl.ds(row(s, k), pos)

    def at(start, size):
        return pl.ds(pl.multiple_of(start, pos), size)

    def seq_rows(chip, s):
        return at((chip * CORES + s) * pos, pos)

    def position(k):
        return at(dev(*slots[k]) * pos, pos)

    barrier = pltpu.get_barrier_semaphore()
    peers = [dev(*o) for o in slots if o != (0, 0)] + [mate]
    for p in peers:
        pl.semaphore_signal(barrier, inc=1, device_id={"seq": p}, device_id_type=MESH)

    wcopies = [pltpu.make_async_copy(ws_hbm.at[position(k)], wm.at[rows(0, k)], wsem.at[k]) for k in range(ns)]
    wcopies += [pltpu.make_async_copy(mk_hbm.at[position(k)], mk.at[rows(0, k)], msem.at[k]) for k in range(ns)]
    own_x = [pltpu.make_async_copy(x_hbm.at[seq_rows(chip_of(0, 0), s)], xa.at[rows(s, home)], xsem.at[s]) for s in range(CORES)]
    own_out = [pltpu.make_async_copy(ob.at[rows(s, home)], out_hbm.at[seq_rows(chip_of(0, 0), s)], outsem.at[s]) for s in range(CORES)]
    wv_copy = pltpu.make_async_copy(wi_hbm.at[:, pl.ds(gate, gate)], wv, vsem)
    wg_copy = pltpu.make_async_copy(wi_hbm.at[:, pl.ds(0, gate)], wg, gsem)
    wo_copy = pltpu.make_async_copy(wo_hbm, wo, osem)
    small = [pltpu.make_async_copy(a, b, psem.at[i]) for i, (a, b) in enumerate((
        (ln1g_hbm, ln1g), (ln1b_hbm, ln1b), (b_in_hbm, b_in), (ln2g_hbm, ln2g), (ln2b_hbm, ln2b), (bsp_hbm, bsp), (b_out_hbm, b_out)))]

    def remote(src, dst, ssem, rsem, target):
        return pltpu.make_async_remote_copy(src_ref=src, dst_ref=dst, send_sem=ssem, recv_sem=rsem,
                                            device_id={"seq": target}, device_id_type=MESH)

    def source(a, s, k):
        return x_hbm.at[seq_rows(chip_of(*slots[k]), s)] if a == 0 else ob.at[rows(s, k)]

    def landing(a, s, k, origin_chip):
        return xa.at[rows(s, k)] if a == 0 else out_hbm.at[seq_rows(origin_chip, s)]

    def message(a, s, k):
        r = back(k)
        return remote(source(a, s, k), landing(a, s, r, chip_of(0, 0)), sent.at[a, s, k], fin.at[a, s, r], dev(*slots[k]))

    def send(a, s, ks):
        for k in ks:
            if k != home:
                message(a, s, k).start()

    def wait_from(a, s, ks):
        for k in ks:
            if k != home:
                remote(source(0, s, home), landing(a, s, k, chip_of(*slots[k])), sent.at[a, s, k], fin.at[a, s, k],
                       mate).wait_recv()

    def swap(s, k):
        return remote(vn.at[s, position(k)], vn.at[s, position(k)], vx_send.at[s, k], vx_recv.at[s, k], mate)

    def wait_swap(s, ks):
        for k in ks:
            da, db = slots[k]
            there = at((chip_of(db, da) * CORES + 1 - c) * pos, pos)
            remote(vn.at[s, position(home)], vn.at[s, there], vx_send.at[s, k], vx_recv.at[s, k], mate).wait_recv()

    accs = (acc0, acc1)
    lnr = 64
    lnr2 = 32

    def ln1(r0, k):
        for r in range(r0, r0 + k, lnr):
            v = xa[r:r + lnr, :].astype(F32)
            cen = v - jnp.sum(v, axis=-1, keepdims=True) * (1.0 / dim)
            var = jnp.sum(cen * cen, axis=-1, keepdims=True) * (1.0 / dim)
            u[r:r + lnr, :] = (cen * lax.rsqrt(var + LN_EPS) * ln1g[...] + ln1b[...]).astype(BF16)

    def steps(hi, product, finish):
        cols = [slice(b, b + NB) for b in range(0, hi, NB)]
        for i in range(len(cols) + 1):
            if i < len(cols):
                raw = product(cols[i])
                k = raw.shape[0]
                accs[i % 2][0:k, :] = raw
            if i > 0:
                finish(cols[i - 1], accs[(i - 1) % 2][0:k, :])

    def value_cols(r0, k):
        def finish(cols, raw):
            bcols = slice(gate + cols.start, gate + cols.stop)
            vbuf[0:k, cols] = gelu(raw + b_in[:, bcols]).astype(BF16)
        steps(gate, lambda cols: dot(u[r0:r0 + k, :], wv[:, cols]), finish)

    def ln2(s, ks):
        for i, k in enumerate(ks):
            v = vbuf[i * pos:(i + 1) * pos, :].astype(F32)
            cen = v - jnp.sum(v, axis=-1, keepdims=True) * (1.0 / gate)
            var = jnp.sum(cen * cen, axis=-1, keepdims=True) * (1.0 / gate)
            vn[s, position(k), :] = (cen * lax.rsqrt(var + LN_EPS) * ln2g[...] + ln2b[...]).astype(BF16)

    def gate_cols(r0, k):
        def finish(cols, raw):
            g[r0:r0 + k, cols] = gelu(raw + b_in[:, cols]).astype(BF16)
        steps(gate, lambda cols: dot(u[r0:r0 + k, :], wg[:, cols]), finish)

    def mask_weights():
        step = 64

        def mask_step(k, carry):
            r = pl.ds(pl.multiple_of(k * step, step), step)
            wm[r, :] = jnp.where(mk[r, :] > 0, wm[r, :].astype(F32), 0.0).astype(BF16)
            return carry
        lax.fori_loop(0, wm.shape[0] // step, mask_step, 0)
        for k in range(bsp.shape[1] // 128):
            blk = jnp.broadcast_to(bsp[:, k * 128:(k + 1) * 128], (128, 128))
            bcol[k * 128:(k + 1) * 128, :] = blk.T
        for k in range(ns):
            bslot[rows(0, k), :] = bcol[position(k), :]

    def spatial(s, w0, k):
        r0 = s * seq + w0

        def finish(cols, raw):
            sp = (raw + bslot[w0:w0 + k, 0:1]).astype(BF16)
            q[0:k, cols] = (g[r0:r0 + k, cols].astype(F32) * sp.astype(F32)).astype(BF16)
        steps(gate, lambda cols: dot(wm[w0:w0 + k, :], vn[s, :, cols]), finish)

    def project(s, w0, k):
        r0 = s * seq + w0

        def finish(cols, raw):
            ob[r0:r0 + k, cols] = (xa[r0:r0 + k, cols].astype(F32) + (raw + b_out[:, cols])).astype(BF16)
        steps(dim, lambda cols: dot(q[0:k, :], wo[:, cols]), finish)

    scope = jax.named_scope

    def front(s, i, k):
        with scope(f"wait0_{s}{i}"):
            if i <= home < i + k:
                own_x[s].wait()
            wait_from(0, s, range(i, i + k))
        with scope(f"ln1_{s}{i}"):
            ln1(s * seq + i * pos, k * pos)
        with scope(f"value_{s}{i}"):
            value_cols(s * seq + i * pos, k * pos)
        with scope(f"ln2_{s}{i}"):
            ln2(s, range(i, i + k))
        for j in range(i, i + k):
            swap(s, j).start()

    def gates(s, i, k):
        with scope(f"gate_{s}{i}"):
            gate_cols(s * seq + i * pos, k * pos)

    def back_part(s, i, k):
        with scope(f"spatial_{s}{i}"):
            spatial(s, i * pos, k * pos)
        with scope(f"project_{s}{i}"):
            project(s, i * pos, k * pos)
        send(1, s, range(i, i + k))
        if i <= home < i + k:
            own_out[s].start()

    for cp in small:
        cp.start()
    for cp in own_x:
        cp.start()
    for cp in wcopies:
        cp.start()
    wv_copy.start()
    wg_copy.start()
    wo_copy.start()
    with scope("barrier"):
        pl.semaphore_wait(barrier, len(peers))
    for s in range(CORES):
        send(0, s, range(ns))
    with scope("mask"):
        for cp in small + wcopies:
            cp.wait()
        mask_weights()
    with scope("w"):
        wv_copy.wait()
        wg_copy.wait()
        wo_copy.wait()
    front(0, 0, 8)
    gates(0, 0, 8)
    front(0, 8, 4)
    front(0, 12, 4)
    gates(0, 8, 8)
    with scope("swap_0"):
        wait_swap(0, range(ns))
    back_part(0, 8, 4)
    back_part(0, 12, 4)
    back_part(0, 0, 8)
    front(1, 0, 8)
    front(1, 8, 8)
    gates(1, 0, 16)
    with scope("swap_1"):
        wait_swap(1, range(ns))
    back_part(1, 8, 4)
    back_part(1, 12, 4)
    back_part(1, 0, 4)
    back_part(1, 4, 4)
    with scope("wait1"):
        wait_from(1, 0, range(ns))
        wait_from(1, 1, range(ns))

    with scope("drain"):
        for s in range(CORES):
            for k in range(ns):
                if k != home:
                    for a in range(2):
                        message(a, s, k).wait_send()
                swap(s, k).wait_send()
            own_out[s].wait()


def solution(mesh):
    n = mesh.shape['seq']
    side = math.isqrt(n // CORES)
    row_spec = P('data', 'seq', None)
    replicated = P()

    def local_block(act_in, ln1_scale, ln1_bias, w_in, b_in, ln2_scale, ln2_bias, w_spatial, b_spatial, causal_mask, w_out, b_out):
        batch, pos, dim = act_in.shape
        gate = w_out.shape[0]
        rows = batch * pos
        seq_len = w_spatial.shape[0]
        ns = side * side
        part = 16 * pos
        if batch != n or side * side * CORES != n:
            raise ValueError('unexpected group')
        anyspec = pl.BlockSpec(memory_space=pl.ANY)
        dma = pltpu.SemaphoreType.DMA
        out = pl.pallas_call(
            functools.partial(kernel, n, side),
            out_shape=pltpu.VMEM((rows, dim), BF16),
            in_specs=[pl.BlockSpec(memory_space=pltpu.HBM)] * 12,
            out_specs=anyspec,
            scratch_shapes=[
                pltpu.VMEM((1, dim), F32), pltpu.VMEM((1, dim), F32), pltpu.VMEM((1, 2 * gate), F32), pltpu.VMEM((1, gate), F32),
                pltpu.VMEM((1, gate), F32), pltpu.VMEM((1, seq_len), F32), pltpu.VMEM((1, dim), F32), dma((7,)),
                pltpu.VMEM((rows, dim), BF16), pltpu.VMEM((rows, dim), BF16),
                pltpu.VMEM((dim, gate), BF16), pltpu.VMEM((dim, gate), BF16), pltpu.VMEM((gate, dim), BF16),
                pltpu.VMEM((ns * pos, seq_len), BF16), pltpu.VMEM((ns * pos, seq_len), jnp.int32),
                pltpu.VMEM((part, gate), BF16),
                pltpu.VMEM((CORES, seq_len, gate), BF16), pltpu.VMEM((rows, gate), BF16),
                pltpu.VMEM((seq_len, 128), F32), pltpu.VMEM((ns * pos, 128), F32),
                pltpu.VMEM((part, gate), BF16), pltpu.VMEM((rows, dim), BF16),
                pltpu.VMEM((part, NB), F32), pltpu.VMEM((part, NB), F32),
                dma((CORES,)), dma, dma((ns,)), dma((ns,)), dma, dma, dma((CORES,)),
                dma((2, CORES, ns)), dma((2, CORES, ns)), dma((CORES, ns)), dma((CORES, ns)),
            ],
            compiler_params=pltpu.CompilerParams(collective_id=0, has_side_effects=True, vmem_limit_bytes=60000000),
            name='gmlp_block',
        )(act_in.reshape(rows, dim), ln1_scale.reshape(1, -1), ln1_bias.reshape(1, -1), w_in, b_in.reshape(1, -1),
          ln2_scale.reshape(1, -1), ln2_bias.reshape(1, -1), w_spatial, b_spatial.reshape(1, -1), causal_mask, w_out,
          b_out.reshape(1, -1))
        return out.reshape(batch, pos, dim)

    return jax.shard_map(local_block, mesh=mesh, in_specs=(row_spec,) + (replicated,) * 11, out_specs=row_spec, check_vma=False)
```

```python
import functools
import math

import jax
import jax.numpy as jnp
from jax import lax
from jax.experimental import pallas as pl
from jax.experimental.pallas import tpu as pltpu
from jax.sharding import PartitionSpec as P

LN_EPS = 1e-6
MESH = pl.DeviceIdType.MESH
F32 = jnp.float32
BF16 = jnp.bfloat16
CORES = 2
NB = 256
GELU_A = math.sqrt(2.0 / math.pi)


def gelu(a):
    return (0.5 * a) * (1.0 + jnp.tanh(a * (GELU_A + (GELU_A * 0.044715) * (a * a))))


def dot(a, b):
    return jnp.dot(a, b, preferred_element_type=F32)


def slot_offsets(side):
    def rank(o):
        da, db = (min(v, side - v) for v in o)
        both = da > 0 and db > 0
        return (both, da != 0 or db != 0, da + db, da > db, o[0] + o[1] != side, o)
    return sorted(((da, db) for da in range(side) for db in range(side)), key=rank)


def kernel(n, side, x_hbm, ln1g_hbm, ln1b_hbm, wi_hbm, b_in_hbm, ln2g_hbm, ln2b_hbm, ws_hbm, bsp_hbm, mk_hbm, wo_hbm, b_out_hbm,
           out_hbm, ln1g, ln1b, b_in, ln2g, ln2b, bsp, b_out, psem,
           xa, u, wv, wg, wo, wm, mk, vbuf, vn, g, bcol, bslot, q, ob,
           acc0, acc1, xsem, vsem, wsem, msem, gsem, osem, outsem, sent, fin, vx_send, vx_recv):
    me = lax.axis_index("seq")
    c = me % CORES
    x = (me // CORES) % side
    y = me // (CORES * side)
    pos = xa.shape[0] // n
    dim = xa.shape[1]
    gate = wo.shape[0]
    slots = slot_offsets(side)
    ns = len(slots)
    home = slots.index((0, 0))
    seq = ns * pos
    fa = x + c * (y - x)
    fb = y + c * (x - y)

    def chip_of(da, db):
        a, b = (fa + da) % side, (fb + db) % side
        yy = b + c * (a - b)
        xx = a + c * (b - a)
        return yy * side + xx

    def dev(da, db):
        return chip_of(da, db) * CORES + c

    mate = me + 1 - 2 * c

    def back(k):
        return slots.index(tuple((side - v) % side for v in slots[k]))

    def row(s, k):
        return s * seq + k * pos

    def rows(s, k):
        return pl.ds(row(s, k), pos)

    def at(start, size):
        return pl.ds(pl.multiple_of(start, pos), size)

    def seq_rows(chip, s):
        return at((chip * CORES + s) * pos, pos)

    def position(k):
        return at(dev(*slots[k]) * pos, pos)

    barrier = pltpu.get_barrier_semaphore()
    peers = [dev(*o) for o in slots if o != (0, 0)] + [mate]
    for p in peers:
        pl.semaphore_signal(barrier, inc=1, device_id={"seq": p}, device_id_type=MESH)

    wcopies = [pltpu.make_async_copy(ws_hbm.at[position(k)], wm.at[rows(0, k)], wsem.at[k]) for k in range(ns)]
    wcopies += [pltpu.make_async_copy(mk_hbm.at[position(k)], mk.at[rows(0, k)], msem.at[k]) for k in range(ns)]
    own_x = [pltpu.make_async_copy(x_hbm.at[seq_rows(chip_of(0, 0), s)], xa.at[rows(s, home)], xsem.at[s]) for s in range(CORES)]
    own_out = [pltpu.make_async_copy(ob.at[rows(s, home)], out_hbm.at[seq_rows(chip_of(0, 0), s)], outsem.at[s]) for s in range(CORES)]
    wv_copy = pltpu.make_async_copy(wi_hbm.at[:, pl.ds(gate, gate)], wv, vsem)
    wg_copy = pltpu.make_async_copy(wi_hbm.at[:, pl.ds(0, gate)], wg, gsem)
    wo_copy = pltpu.make_async_copy(wo_hbm, wo, osem)
    small = [pltpu.make_async_copy(a, b, psem.at[i]) for i, (a, b) in enumerate((
        (ln1g_hbm, ln1g), (ln1b_hbm, ln1b), (b_in_hbm, b_in), (ln2g_hbm, ln2g), (ln2b_hbm, ln2b), (bsp_hbm, bsp), (b_out_hbm, b_out)))]

    def remote(src, dst, ssem, rsem, target):
        return pltpu.make_async_remote_copy(src_ref=src, dst_ref=dst, send_sem=ssem, recv_sem=rsem,
                                            device_id={"seq": target}, device_id_type=MESH)

    def source(a, s, k):
        return x_hbm.at[seq_rows(chip_of(*slots[k]), s)] if a == 0 else ob.at[rows(s, k)]

    def landing(a, s, k, origin_chip):
        return xa.at[rows(s, k)] if a == 0 else out_hbm.at[seq_rows(origin_chip, s)]

    def message(a, s, k):
        r = back(k)
        return remote(source(a, s, k), landing(a, s, r, chip_of(0, 0)), sent.at[a, s, k], fin.at[a, s, r], dev(*slots[k]))

    def send(a, s, ks):
        for k in ks:
            if k != home:
                message(a, s, k).start()

    def wait_from(a, s, ks):
        for k in ks:
            if k != home:
                remote(source(0, s, home), landing(a, s, k, chip_of(*slots[k])), sent.at[a, s, k], fin.at[a, s, k],
                       mate).wait_recv()

    def swap(s, k):
        return remote(vn.at[s, position(k)], vn.at[s, position(k)], vx_send.at[s, k], vx_recv.at[s, k], mate)

    def wait_swap(s, ks):
        for k in ks:
            da, db = slots[k]
            there = at((chip_of(db, da) * CORES + 1 - c) * pos, pos)
            remote(vn.at[s, position(home)], vn.at[s, there], vx_send.at[s, k], vx_recv.at[s, k], mate).wait_recv()

    accs = (acc0, acc1)
    lnr = 64
    lnr2 = 32

    def ln1(r0, k):
        for r in range(r0, r0 + k, lnr):
            v = xa[r:r + lnr, :].astype(F32)
            cen = v - jnp.sum(v, axis=-1, keepdims=True) * (1.0 / dim)
            var = jnp.sum(cen * cen, axis=-1, keepdims=True) * (1.0 / dim)
            u[r:r + lnr, :] = (cen * lax.rsqrt(var + LN_EPS) * ln1g[...] + ln1b[...]).astype(BF16)

    def steps(hi, product, finish):
        cols = [slice(b, b + NB) for b in range(0, hi, NB)]
        for i in range(len(cols) + 1):
            if i < len(cols):
                raw = product(cols[i])
                k = raw.shape[0]
                accs[i % 2][0:k, :] = raw
            if i > 0:
                finish(cols[i - 1], accs[(i - 1) % 2][0:k, :])

    def value_cols(r0, k):
        def finish(cols, raw):
            bcols = slice(gate + cols.start, gate + cols.stop)
            vbuf[0:k, cols] = gelu(raw + b_in[:, bcols]).astype(BF16)
        steps(gate, lambda cols: dot(u[r0:r0 + k, :], wv[:, cols]), finish)

    def ln2(s, ks):
        for i, k in enumerate(ks):
            v = vbuf[i * pos:(i + 1) * pos, :].astype(F32)
            cen = v - jnp.sum(v, axis=-1, keepdims=True) * (1.0 / gate)
            var = jnp.sum(cen * cen, axis=-1, keepdims=True) * (1.0 / gate)
            vn[s, position(k), :] = (cen * lax.rsqrt(var + LN_EPS) * ln2g[...] + ln2b[...]).astype(BF16)

    def gate_cols(r0, k):
        def finish(cols, raw):
            g[r0:r0 + k, cols] = gelu(raw + b_in[:, cols]).astype(BF16)
        steps(gate, lambda cols: dot(u[r0:r0 + k, :], wg[:, cols]), finish)

    def mask_weights():
        step = 64

        def mask_step(k, carry):
            r = pl.ds(pl.multiple_of(k * step, step), step)
            wm[r, :] = jnp.where(mk[r, :] > 0, wm[r, :].astype(F32), 0.0).astype(BF16)
            return carry
        lax.fori_loop(0, wm.shape[0] // step, mask_step, 0)
        for k in range(bsp.shape[1] // 128):
            blk = jnp.broadcast_to(bsp[:, k * 128:(k + 1) * 128], (128, 128))
            bcol[k * 128:(k + 1) * 128, :] = blk.T
        for k in range(ns):
            bslot[rows(0, k), :] = bcol[position(k), :]

    def spatial(s, w0, k):
        r0 = s * seq + w0

        def finish(cols, raw):
            sp = (raw + bslot[w0:w0 + k, 0:1]).astype(BF16)
            q[0:k, cols] = (g[r0:r0 + k, cols].astype(F32) * sp.astype(F32)).astype(BF16)
        steps(gate, lambda cols: dot(wm[w0:w0 + k, :], vn[s, :, cols]), finish)

    def project(s, w0, k):
        r0 = s * seq + w0

        def finish(cols, raw):
            ob[r0:r0 + k, cols] = (xa[r0:r0 + k, cols].astype(F32) + (raw + b_out[:, cols])).astype(BF16)
        steps(dim, lambda cols: dot(q[0:k, :], wo[:, cols]), finish)

    scope = jax.named_scope

    def front(s, i, k):
        with scope(f"wait0_{s}{i}"):
            if i <= home < i + k:
                own_x[s].wait()
            wait_from(0, s, range(i, i + k))
        with scope(f"ln1_{s}{i}"):
            ln1(s * seq + i * pos, k * pos)
        with scope(f"value_{s}{i}"):
            value_cols(s * seq + i * pos, k * pos)
        with scope(f"ln2_{s}{i}"):
            ln2(s, range(i, i + k))
        for j in range(i, i + k):
            swap(s, j).start()

    def gates(s, i, k):
        with scope(f"gate_{s}{i}"):
            gate_cols(s * seq + i * pos, k * pos)

    def back_part(s, i, k):
        with scope(f"spatial_{s}{i}"):
            spatial(s, i * pos, k * pos)
        with scope(f"project_{s}{i}"):
            project(s, i * pos, k * pos)
        send(1, s, range(i, i + k))
        if i <= home < i + k:
            own_out[s].start()

    for cp in small:
        cp.start()
    for cp in own_x:
        cp.start()
    for cp in wcopies:
        cp.start()
    wv_copy.start()
    wg_copy.start()
    wo_copy.start()
    with scope("barrier"):
        pl.semaphore_wait(barrier, len(peers))
    send(0, 0, range(ns))
    with scope("mask"):
        for cp in small + wcopies:
            cp.wait()
        mask_weights()
    with scope("w"):
        wv_copy.wait()
        wg_copy.wait()
        wo_copy.wait()
    front(0, 0, 8)
    send(0, 1, range(ns))
    gates(0, 0, 8)
    front(0, 8, 4)
    front(0, 12, 4)
    gates(0, 8, 8)
    with scope("swap_0"):
        wait_swap(0, range(ns))
    back_part(0, 8, 4)
    back_part(0, 12, 4)
    back_part(0, 0, 8)
    front(1, 0, 8)
    front(1, 8, 8)
    gates(1, 0, 16)
    with scope("swap_1"):
        wait_swap(1, range(ns))
    back_part(1, 8, 4)
    back_part(1, 12, 4)
    back_part(1, 0, 4)
    back_part(1, 4, 4)
    with scope("wait1"):
        wait_from(1, 0, range(ns))
        wait_from(1, 1, range(ns))

    with scope("drain"):
        for s in range(CORES):
            for k in range(ns):
                if k != home:
                    for a in range(2):
                        message(a, s, k).wait_send()
                swap(s, k).wait_send()
            own_out[s].wait()


def solution(mesh):
    n = mesh.shape['seq']
    side = math.isqrt(n // CORES)
    row_spec = P('data', 'seq', None)
    replicated = P()

    def local_block(act_in, ln1_scale, ln1_bias, w_in, b_in, ln2_scale, ln2_bias, w_spatial, b_spatial, causal_mask, w_out, b_out):
        batch, pos, dim = act_in.shape
        gate = w_out.shape[0]
        rows = batch * pos
        seq_len = w_spatial.shape[0]
        ns = side * side
        part = 16 * pos
        if batch != n or side * side * CORES != n:
            raise ValueError('unexpected group')
        anyspec = pl.BlockSpec(memory_space=pl.ANY)
        dma = pltpu.SemaphoreType.DMA
        out = pl.pallas_call(
            functools.partial(kernel, n, side),
            out_shape=pltpu.VMEM((rows, dim), BF16),
            in_specs=[pl.BlockSpec(memory_space=pltpu.HBM)] * 12,
            out_specs=anyspec,
            scratch_shapes=[
                pltpu.VMEM((1, dim), F32), pltpu.VMEM((1, dim), F32), pltpu.VMEM((1, 2 * gate), F32), pltpu.VMEM((1, gate), F32),
                pltpu.VMEM((1, gate), F32), pltpu.VMEM((1, seq_len), F32), pltpu.VMEM((1, dim), F32), dma((7,)),
                pltpu.VMEM((rows, dim), BF16), pltpu.VMEM((rows, dim), BF16),
                pltpu.VMEM((dim, gate), BF16), pltpu.VMEM((dim, gate), BF16), pltpu.VMEM((gate, dim), BF16),
                pltpu.VMEM((ns * pos, seq_len), BF16), pltpu.VMEM((ns * pos, seq_len), jnp.int32),
                pltpu.VMEM((part, gate), BF16),
                pltpu.VMEM((CORES, seq_len, gate), BF16), pltpu.VMEM((rows, gate), BF16),
                pltpu.VMEM((seq_len, 128), F32), pltpu.VMEM((ns * pos, 128), F32),
                pltpu.VMEM((part, gate), BF16), pltpu.VMEM((rows, dim), BF16),
                pltpu.VMEM((part, NB), F32), pltpu.VMEM((part, NB), F32),
                dma((CORES,)), dma, dma((ns,)), dma((ns,)), dma, dma, dma((CORES,)),
                dma((2, CORES, ns)), dma((2, CORES, ns)), dma((CORES, ns)), dma((CORES, ns)),
            ],
            compiler_params=pltpu.CompilerParams(collective_id=0, has_side_effects=True, vmem_limit_bytes=60000000),
            name='gmlp_block',
        )(act_in.reshape(rows, dim), ln1_scale.reshape(1, -1), ln1_bias.reshape(1, -1), w_in, b_in.reshape(1, -1),
          ln2_scale.reshape(1, -1), ln2_bias.reshape(1, -1), w_spatial, b_spatial.reshape(1, -1), causal_mask, w_out,
          b_out.reshape(1, -1))
        return out.reshape(batch, pos, dim)

    return jax.shard_map(local_block, mesh=mesh, in_specs=(row_spec,) + (replicated,) * 11, out_specs=row_spec, check_vma=False)
```
